32 devices in a mesh: groups: 2 (over y), tp: 4 (over z), seq: 4 (over x, core).
Axes of the slice: x: 2, y: 2, z: 4, core: 2. Of those that a mesh axis runs over, the one named last changes fastest.
Arguments:
- kv_prefill: bfloat16 [2, 2, 8, 32768, 128], P(None, None, 'groups', ('tp', 'seq')), parts along dimension 2, may hold values from -10 to 10
- queries: bfloat16 [2, 8, 64, 128], P(None, ('groups', 'seq'), 'tp'), parts along dimension 1, may hold values from -512 to 512
- new_kv: bfloat16 [2, 2, 8, 8, 128], P(None, None, ('groups', 'seq')), parts along dimension 2, may hold values from -4.5 to 4.5
- lengths: int32 [8], P(('groups', 'seq')), parts along dimension 0, may hold values from 2048 to 4095
- page_slots: int32 [8, 256], P(('groups', 'seq')), parts along dimension 0, may hold values from 0 to 255, each once within a row
Outputs:
- decode_pool: bfloat16 [2, 2, 8, 2048, 16, 128], P(None, None, 'tp', ('groups', 'seq')), parts along dimension 3
- attention_out: bfloat16 [2, 8, 64, 128], P(None, ('groups', 'seq'), 'tp'), parts along dimension 1
The draws below stay inside these ranges and needn't reach their ends.
There are 2 independent parts, one for each index of `groups`. The reference program is written for one: setup_inputs(seed, part) draws one part's arguments, and reference() takes and returns one part's arrays. A program takes and returns all parts, laid end to end along the dimension named above; each array names one. Nothing has to cross between parts.
Inputs may be any that keep to these rules, and one draw needn't show every extreme that they name: Row b belongs to sequence b: its page j goes to slot page_slots[b, j] of the row's block of 256 slots; each row uses every slot once.
All inputs are finite; a program needn't handle non-finite values.
Results may differ from the reference program's by a relative error of at most 0.01.
Values may be sent and summed in bfloat16 or wider, within the bound.
A program may use at most 64 MiB of HBM per device.

```python
import math
import jax
import jax.numpy as jnp
from jax import lax

LAYERS = 2
KVH = 8
QH = 64
DH = 128
PAGE = 16
CTX = 4096
SEQ_DEV = 1
SEQS = 4
PAGES = 256
COPIES = 8


def cache_and_query(key):
    cache_shape = (2, LAYERS, SEQS, KVH, CTX, DH)
    base_cache = jax.random.truncated_normal(jax.random.fold_in(key, 101), -4.5, 4.5, cache_shape, jnp.float32)
    base_query = jax.random.truncated_normal(jax.random.fold_in(key, 102), -4.5, 4.5, (LAYERS, SEQS, KVH, QH // KVH, DH), jnp.float32)
    cache_rows = base_cache
    query_rows = base_query
    return (cache_rows.reshape(2, LAYERS, SEQS, KVH * CTX, DH), query_rows.reshape(LAYERS, SEQS, QH, DH))


def draw_kv_prefill(key, part):
    return cache_and_query(key)[0].astype(jnp.bfloat16)


def draw_queries(key, part):
    return cache_and_query(key)[1].astype(jnp.bfloat16)


def with_ends(entries, stream_key, smallest, top_value):
    dims = entries.shape
    place = [jax.random.randint(jax.random.fold_in(stream_key, axis), (), 0, dims[axis]) for axis in range(len(dims))]
    entries = entries.at[tuple(place)].set(smallest)
    longest = dims.index(max(dims))
    place[longest] = (place[longest] + 1) % dims[longest]
    return entries.at[tuple(place)].set(top_value)


def block_scale(rng, shape, split, low, largest):
    factor_of = 1.0
    for axis_at, blocks in split:
        draws = jax.random.uniform(jax.random.fold_in(jax.random.fold_in(rng, 6), axis_at), (blocks,), jnp.float32, low / len(split), largest / len(split))
        factor_of = factor_of * jnp.repeat(jnp.exp(draws), shape[axis_at] // blocks).reshape((-1,) + (1,) * (len(shape) - 1 - axis_at))
    return factor_of


def gaussian(key, dims, scale, most, split=(), held_as=jnp.bfloat16):
    values = jax.random.normal(key, dims, jnp.float32) * scale
    if len(split) > 0:
        values = block_scale(key, dims, split, -0.22, 0.18) * values
    return jnp.clip(values, min=-most, max=most).astype(held_as)


def setup_inputs(seed: int = 0, part: int = 0) -> dict:
    seeds = jax.random.split(jax.random.key(seed), 6)
    own_keys = jax.random.split(jax.random.fold_in(seeds[5], part), 6)
    return {
        "kv_prefill": draw_kv_prefill(jax.random.fold_in(jax.random.fold_in(seeds[5], part), 71), part),
        "queries": draw_queries(jax.random.fold_in(jax.random.fold_in(seeds[5], part), 71), part),
        "new_kv": gaussian(own_keys[2], (2, LAYERS, SEQS, KVH, DH), 1.0, 4.5, ((2, 4),)),
        "lengths": with_ends(jax.random.randint(own_keys[3], (SEQS,), CTX // 2, CTX), jax.random.fold_in(own_keys[3], 1), CTX // 2, CTX - 1).astype(jnp.int32),
        "page_slots": jax.vmap(lambda own: jax.random.permutation(own, SEQ_DEV * PAGES))(jax.random.split(own_keys[4], (SEQS // SEQ_DEV))).reshape((SEQS // SEQ_DEV, SEQ_DEV * PAGES)).astype(jnp.int32),
    }


def reference(kv_prefill, queries, new_kv, lengths, page_slots):
    positions = jnp.arange(CTX, dtype=jnp.int32)
    arriving = positions[None, :] == lengths[:, None]
    cache_full = kv_prefill.reshape(2, LAYERS, SEQS, KVH, CTX, DH)
    cache_full = jnp.where(arriving[None, None, :, None, :, None], new_kv[:, :, :, :, None, :], cache_full)
    slots_block = SEQ_DEV * PAGES
    owners = jnp.arange(SEQS * PAGES, dtype=jnp.int32) // slots_block
    slot_index = owners * slots_block + page_slots.reshape(-1).astype(jnp.int32)
    paged_rows = cache_full.reshape(2, LAYERS, SEQS, KVH, PAGES, PAGE, DH).transpose(0, 1, 3, 2, 4, 5, 6)
    paged_rows = paged_rows.reshape(2, LAYERS, KVH, SEQS * PAGES, PAGE, DH)
    by_head = jnp.zeros_like(paged_rows).at[:, :, :, slot_index].set(paged_rows)
    copy_heads = jnp.arange(COPIES, dtype=jnp.int32) * KVH // COPIES
    decode_pool = jnp.take(by_head, copy_heads, axis=2)
    key_cache = cache_full[0].astype(jnp.float32)
    value_cache = cache_full[1].astype(jnp.float32)
    grouped_q = queries.astype(jnp.float32).reshape(LAYERS, SEQS, KVH, QH // KVH, DH)
    scores = jnp.einsum('lshgd,lshtd->lshgt', grouped_q, key_cache, precision=lax.Precision.HIGHEST) * (1.0 / math.sqrt(DH))
    visible = (positions[None, :] <= lengths[:, None])[None, :, None, None, :]
    masked = jnp.where(visible, scores, -1e+30)
    highest = lax.optimization_barrier(jnp.max(masked, axis=-1, keepdims=True))
    exponent = jnp.where(visible, jnp.exp(masked - highest), 0.0)
    weights = (exponent / lax.optimization_barrier(jnp.sum(exponent, axis=-1, keepdims=True))).astype(jnp.bfloat16)
    mixed_out = jnp.einsum('lshgt,lshtd->lshgd', weights.astype(jnp.float32), value_cache, precision=lax.Precision.HIGHEST)
    attention_out = mixed_out.astype(jnp.bfloat16).reshape(LAYERS, SEQS, QH, DH)
    return (decode_pool, attention_out)
```

```python
import functools
import math

import jax
import jax.numpy as jnp
from jax import lax
from jax.experimental import pallas as pl
from jax.experimental.pallas import tpu as pltpu
from jax.sharding import PartitionSpec as P

PAGE = 16
UNROLL = 16


def swapped(array, axis, bits):
    return lax.ppermute(array, axis, [(i, i ^ bits) for i in range(lax.axis_size(axis))])


def spread_heads(blocks, fanout):
    rank = lax.axis_index("tp")
    for bit in range(fanout.bit_length() - 1):
        partner = swapped(blocks, "tp", 1 << bit)
        lower = rank // (1 << bit) % 2 == 0
        pair = (jnp.where(lower, blocks, partner), jnp.where(lower, partner, blocks))
        blocks = jnp.concatenate(pair, axis=3)
    return blocks


def head_kernel(
    units, group, own, sources, fanout, heads, tp_ranks, kv_heads, has_pool, earlier, *refs
):
    refs = list(refs)
    slots, lengths, queries, fresh = refs[:4]
    refs = refs[4:]
    own_ref = refs.pop(0) if own else None
    piece_count = sources - 1 if own else sources
    pieces = [[refs.pop(0) for _ in range(piece_count)] for _ in units]
    keys = [u for u in units if u[0] == 0]
    value_layers = [u[1] for u in units if u[0] == 1]
    outer_probs = {l: refs.pop(0) for l in value_layers if (0, l) not in keys}
    all_sums = {name: refs.pop(0) for name in earlier or ()}
    if has_pool:
        refs.pop(0)
    pool = refs.pop(0)
    made_probs = {l: refs.pop(0) for _, l in keys if l not in value_layers}
    mixed = {}
    if earlier is None:
        mixed = {l: refs.pop(0) for l in value_layers}
    else:
        attention_out = refs.pop(0)
    cache, paged, in_sems, out_sems = refs

    me = lax.axis_index("seq")
    mine = me % sources
    head = (me // sources) ^ group
    first = lax.axis_index("tp") * kv_heads // tp_ranks
    copies = []
    for n, (k, l) in enumerate(units):
        for e in range(sources):
            if own and e == 0:
                source = own_ref.at[k, l, me]
            else:
                source = pieces[n][e - 1 if own else e]
            copies.append(
                pltpu.make_async_copy(source, cache.at[n, :, mine ^ e], in_sems.at[n, e])
            )
            copies[-1].start()

    length = lengths[0]
    blocks = cache.shape[3]
    pages = fanout * sources * blocks
    positions = pages * PAGE
    depth = cache.shape[-1]
    at_page = length // PAGE
    probs_now = {}
    flushes = []
    for n, (k, l) in enumerate(units):
        for e in range(sources):
            copies[n * sources + e].wait()
        rows = fresh[k, l, 0].astype(jnp.float32)
        row_at = lax.broadcasted_iota(jnp.int32, rows.shape, 0)
        row = jnp.sum(jnp.where(row_at == first + head, rows, 0.0), axis=0, keepdims=True)
        spot = (n, at_page // (sources * blocks), at_page // blocks % sources, at_page % blocks)
        page = cache[spot].astype(jnp.float32)
        offset = lax.broadcasted_iota(jnp.int32, page.shape, 0)
        cache[spot] = jnp.where(offset == length % PAGE, row, page).astype(cache.dtype)

        def move(step, carry):
            start = step * UNROLL
            held = []
            for i in range(UNROLL):
                j = start + i
                held.append(cache[n, j // (sources * blocks), j // blocks % sources, j % blocks])
            for i in range(UNROLL):
                paged[n, slots[0, start + i]] = held[i]
            return carry

        lax.fori_loop(0, pages // UNROLL, move, 0)
        flush = pltpu.make_async_copy(paged.at[n], pool.at[k, l, head], out_sems.at[n])
        flush.start()
        flushes.append(flush)

        rows_all = cache[n].reshape(positions, depth)
        if k == 0:
            query = queries[l, head]
            scores = lax.dot_general(
                query, rows_all, (((1,), (1,)), ((), ())), preferred_element_type=jnp.float32
            ) * (1.0 / math.sqrt(depth))
            visible = lax.broadcasted_iota(jnp.int32, scores.shape, 1) <= length
            masked = jnp.where(visible, scores, -1e30)
            highest = jnp.max(masked, axis=-1, keepdims=True)
            exponent = jnp.where(visible, jnp.exp(masked - highest), 0.0)
            total = jnp.sum(exponent, axis=-1, keepdims=True)
            probs = (exponent / total).astype(jnp.bfloat16)
            if l in made_probs:
                made_probs[l][...] = probs
            else:
                probs_now[l] = probs
        else:
            probs = probs_now[l] if l in probs_now else outer_probs[l][...]
            weighted = jnp.dot(probs, rows_all, preferred_element_type=jnp.float32)
            if earlier is None:
                mixed[l][...] = weighted
            else:
                all_sums[group, l] = weighted
    if earlier is not None:
        for l in range(queries.shape[0]):
            for h in range(heads):
                mine_now = jnp.zeros((queries.shape[2], depth), jnp.float32)
                for g in range(heads):
                    picked = (me // sources) ^ g == h
                    mine_now = jnp.where(picked, all_sums[g, l][...], mine_now)
                here = pl.ds(h * queries.shape[2], queries.shape[2])
                attention_out[l, here, :] = mine_now.astype(attention_out.dtype)
    for flush in flushes:
        flush.wait()


def head_call(units, group, own, pieces, probs, pool, pool_shape, args, sizes, sums):
    slots, lengths, queries, fresh, own_ref = args
    sources, fanout, heads, tp_ranks, blocks, depth = sizes
    per_head = queries.shape[2]
    pages = fanout * sources * blocks
    smem = pl.BlockSpec(memory_space=pltpu.SMEM)
    vmem = pl.BlockSpec(memory_space=pltpu.VMEM)
    anywhere = pl.BlockSpec(memory_space=pl.ANY)
    operands = [slots, lengths, queries, fresh]
    in_specs = [smem, smem, vmem, vmem]
    if own:
        operands.append(own_ref)
        in_specs.append(anywhere)
    for of_unit in pieces:
        operands += of_unit
        in_specs += [anywhere] * len(of_unit)
    key_layers = [l for k, l in units if k == 0]
    value_layers = [l for k, l in units if k == 1]
    for l in value_layers:
        if l not in key_layers:
            operands.append(probs[l])
            in_specs.append(vmem)
    earlier = None if sums is None else list(sums)
    for name in earlier or ():
        operands.append(sums[name])
        in_specs.append(vmem)
    aliases = {}
    if pool is not None:
        aliases = {len(operands): 0}
        operands.append(pool)
        in_specs.append(anywhere)
    made = [l for l in key_layers if l not in value_layers]
    out_shape = [jax.ShapeDtypeStruct(pool_shape, jnp.bfloat16)]
    out_shape += [jax.ShapeDtypeStruct((per_head, pages * PAGE), jnp.bfloat16)] * len(made)
    if sums is None:
        out_shape += [jax.ShapeDtypeStruct((per_head, depth), jnp.float32)] * len(value_layers)
    else:
        rows = (queries.shape[0], heads * per_head, depth)
        out_shape.append(jax.ShapeDtypeStruct(rows, jnp.bfloat16))
    unit_bytes = pages * PAGE * depth * 2
    results = pl.pallas_call(
        functools.partial(
            head_kernel, units, group, own, sources, fanout, heads, tp_ranks,
            fresh.shape[3], pool is not None, earlier,
        ),
        out_shape=out_shape,
        in_specs=in_specs,
        out_specs=[anywhere] + [vmem] * (len(out_shape) - 1),
        scratch_shapes=[
            pltpu.VMEM((len(units), fanout, sources, blocks, PAGE, depth), jnp.bfloat16),
            pltpu.VMEM((len(units), pages, PAGE, depth), jnp.bfloat16),
            pltpu.SemaphoreType.DMA((len(units), sources)),
            pltpu.SemaphoreType.DMA((len(units),)),
        ],
        input_output_aliases=aliases,
        compiler_params=pltpu.CompilerParams(vmem_limit_bytes=24 << 20),
        cost_estimate=pl.CostEstimate(
            flops=len(units) * 2 * per_head * pages * PAGE * depth,
            bytes_accessed=len(units) * 2 * unit_bytes,
            transcendentals=0,
        ),
    )(*operands)
    pool = results[0]
    rest = list(results[1:])
    new_probs = {l: rest.pop(0) for l in made}
    if sums is not None:
        return pool, new_probs, rest.pop(0)
    return pool, new_probs, {l: rest.pop(0) for l in value_layers}


def body(tp_ranks, seq_ranks, kv_prefill, queries, new_kv, lengths, page_slots):
    kv_heads = new_kv.shape[3]
    layers = kv_prefill.shape[1]
    depth = kv_prefill.shape[4]
    heads = max(1, kv_heads // tp_ranks)
    fanout = tp_ranks * heads // kv_heads
    sources = seq_ranks // heads
    blocks = kv_prefill.shape[3] // PAGE
    pages = page_slots.shape[1]
    me = lax.axis_index("seq")

    spread = spread_heads(kv_prefill, fanout)
    spread = spread.reshape(2, layers, spread.shape[2], fanout, blocks, PAGE, depth)
    units = [(k, l) for k in (0, 1) for l in range(layers)]

    arrived = {}
    left = spread
    for k, l in units:
        deltas = range(sources, seq_ranks) if heads > 1 else range(1, sources)
        if (k, l) == units[1] and heads > 1:
            deltas = [*deltas, *range(1, sources)]
            near = units
        else:
            near = ()
        blocks_out = {}
        for delta in deltas:
            for at in near if delta < sources and heads > 1 else ((k, l),):
                start = (*at, me ^ delta, 0, 0, 0, 0)
                size = (1, 1, 1, *spread.shape[3:])
                blocks_out[delta, *at] = lax.dynamic_slice(left, start, size)
        names = list(blocks_out)
        values, left = lax.optimization_barrier(([blocks_out[n] for n in names], left))
        for name, value in zip(names, values):
            arrived[name] = swapped(value.reshape(spread.shape[3:]), "seq", name[0])

    grouped = queries.reshape(layers, heads, queries.shape[2] // heads, depth)
    args = (page_slots, lengths, grouped, new_kv, spread)
    sizes = (sources, fanout, heads, tp_ranks, blocks, depth)
    pool_shape = (2, layers, heads, pages, PAGE, depth)
    pieces = [[arrived[e, k, l] for e in range(1, sources)] for k, l in units]
    pool, _, mixed = head_call(
        units, 0, True, pieces, {}, None, pool_shape, args, sizes, None if heads > 1 else {}
    )
    sums = {}
    if heads > 1:
        sums = {(0, l): mixed[l] for l in mixed}
    probs = {}
    for group in range(1, heads):
        for k, l in units:
            last = group == heads - 1 and (k, l) == units[-1]
            piece = [arrived[group * sources + e, k, l] for e in range(sources)]
            pool, made, mixed = head_call(
                [(k, l)], group, False, [piece], {l: probs.get((group, l))},
                pool, pool_shape, args, sizes, sums if last else None,
            )
            for at, value in made.items():
                probs[group, at] = value
            if not last:
                sums.update({(group, at): value for at, value in mixed.items()})
    return pool, mixed.reshape(queries.shape)


def solution(mesh):
    placed = (
        P(None, None, "groups", ("tp", "seq"), None),
        P(None, ("groups", "seq"), "tp", None),
        P(None, None, ("groups", "seq"), None, None),
        P(("groups", "seq")),
        P(("groups", "seq"), None),
    )
    return jax.shard_map(
        functools.partial(body, mesh.shape["tp"], mesh.shape["seq"]),
        mesh=mesh,
        in_specs=placed,
        out_specs=(
            P(None, None, "tp", ("groups", "seq"), None, None),
            P(None, ("groups", "seq"), "tp", None),
        ),
        check_vma=False,
    )
```

```python
import functools
import math

import jax
import jax.numpy as jnp
from jax import lax
from jax.experimental import pallas as pl
from jax.experimental.pallas import tpu as pltpu
from jax.sharding import PartitionSpec as P


PAGE = 16
UNROLL = 16


def swapped(array, axis, bits):
    return lax.ppermute(array, axis, [(i, i ^ bits) for i in range(lax.axis_size(axis))])


def spread_heads(blocks, fanout):
    rank = lax.axis_index("tp")
    for bit in range(fanout.bit_length() - 1):
        partner = swapped(blocks, "tp", 1 << bit)
        lower = rank // (1 << bit) % 2 == 0
        pair = (jnp.where(lower, blocks, partner), jnp.where(lower, partner, blocks))
        blocks = jnp.concatenate(pair, axis=3)
    return blocks


def cut_kernel(wanted, *refs):
    spread, outs, sems = refs[0], refs[-1 - len(wanted) : -1], refs[-1]
    me = lax.axis_index("seq")
    copies = []
    for out, items in zip(outs, wanted):
        for n, (k, l, delta, lo, hi) in enumerate(items):
            source = spread.at[k, l, me ^ delta, :, lo:hi]
            copies.append(pltpu.make_async_copy(source, out.at[n], sems.at[len(copies)]))
            copies[-1].start()
    for copy in copies:
        copy.wait()


def cut(spread, wanted, after):
    fanout, _, page, depth = spread.shape[3:]
    shapes = [
        jax.ShapeDtypeStruct((len(w), fanout, w[0][4] - w[0][3], page, depth), spread.dtype)
        for w in wanted
    ]
    anywhere = pl.BlockSpec(memory_space=pl.ANY)
    return pl.pallas_call(
        functools.partial(cut_kernel, wanted),
        out_shape=shapes,
        in_specs=[pl.BlockSpec(memory_space=pltpu.HBM)] + [anywhere] * len(after),
        out_specs=[pl.BlockSpec(memory_space=pltpu.VMEM)] * len(shapes),
        scratch_shapes=[pltpu.SemaphoreType.DMA((sum(len(w) for w in wanted),))],
        compiler_params=pltpu.CompilerParams(vmem_limit_bytes=8 << 20),
        cost_estimate=pl.CostEstimate(
            flops=0, bytes_accessed=2 * sum(2 * math.prod(o.shape) for o in shapes), transcendentals=0
        ),
    )(spread, *after)


def head_kernel(plan, *refs):
    refs = list(refs)

    def take(count):
        return [refs.pop(0) for _ in range(count)]

    units, group, sources = plan["units"], plan["group"], plan["sources"]
    slots, lengths, queries, fresh = take(4)
    own_ref = take(1)[0] if plan["own"] else None
    operands = take(plan["operands"])
    given_probs = dict(zip(plan["given_probs"], take(len(plan["given_probs"]))))
    sums_in = dict(zip(plan["sums_in"], take(len(plan["sums_in"]))))
    if plan["has_pool"]:
        take(1)
    (pool,) = take(1)
    probs_out = dict(zip(plan["probs_out"], take(len(plan["probs_out"]))))
    sums_out = dict(zip(plan["sums_out"], take(len(plan["sums_out"]))))
    attention_out = take(1)[0] if plan["final"] else None
    scores, paged, own_buf, in_sems, out_sems = refs

    me = lax.axis_index("seq")
    mine = me % sources
    head = (me // sources) ^ group
    heads = plan["heads"]
    first = lax.axis_index("tp") * plan["kv_heads"] // plan["tp_ranks"]
    fanout, blocks, _, depth = plan["piece"]
    length = lengths[0]
    per_head = queries.shape[2]
    places = lax.broadcasted_iota(jnp.int32, scores.shape, 0) * (blocks * PAGE)
    places += lax.broadcasted_iota(jnp.int32, scores.shape, 2)
    fetches = []
    if plan["own"]:
        for n, (k, l) in enumerate(units):
            fetches.append(
                pltpu.make_async_copy(own_ref.at[k, l, me], own_buf.at[n], in_sems.at[n])
            )
            fetches[-1].start()

    probs_now = dict(given_probs)
    sums = dict(sums_in)
    flushes = []
    for n, (k, l) in enumerate(units):
        parts = []
        if plan["own"]:
            fetches[n].wait()
            parts.append((own_buf.at[n], 0, 0, blocks))
        parts += [
            (operands[at].at[row], e, lo, hi)
            for at, row, unit, e, lo, hi in plan["parts"]
            if unit == (k, l)
        ]
        rows = fresh[k, l, 0].astype(jnp.float32)
        row_at = lax.broadcasted_iota(jnp.int32, rows.shape, 0)
        row = jnp.sum(jnp.where(row_at == first + head, rows, 0.0), axis=0, keepdims=True)

        def patched(page):
            offset = lax.broadcasted_iota(jnp.int32, page.shape, 0)
            return jnp.where(offset == length % PAGE, row, page.astype(jnp.float32)).astype(page.dtype)

        if plan["close"]:
            count = 0
            for ref, e, lo, hi in parts:
                for f in range(fanout):
                    base = (f * sources + (mine ^ e)) * blocks + lo
                    paged[n, count : count + hi - lo] = ref[f]
                    inside = (length // PAGE >= base) & (length // PAGE < base + hi - lo)

                    @pl.when(inside)
                    def _():
                        at = count + length // PAGE - base
                        paged[n, at] = patched(paged[n, at])

                    for b in range(hi - lo):
                        pltpu.make_async_copy(
                            paged.at[n, count + b],
                            pool.at[k, l, head, slots[0, base + b]],
                            out_sems.at[n],
                        ).start()
                    count += hi - lo
            done = pltpu.make_async_copy(
                paged.at[n, :count], pool.at[k, l, head, :count], out_sems.at[n]
            )
        else:
            for ref, e, lo, hi in parts:
                for f in range(fanout):
                    base = (f * sources + (mine ^ e)) * blocks + lo
                    unroll = math.gcd(UNROLL, hi - lo)

                    def move(step, carry, ref=ref, f=f, base=base, unroll=unroll):
                        start = step * unroll
                        held = [ref[f, start + i] for i in range(unroll)]
                        for i in range(unroll):
                            paged[n, slots[0, base + start + i]] = held[i]
                        return carry

                    lax.fori_loop(0, (hi - lo) // unroll, move, 0)
            spot = slots[0, length // PAGE]
            paged[n, spot] = patched(paged[n, spot])
            done = pltpu.make_async_copy(paged.at[n], pool.at[k, l, head], out_sems.at[n])
            done.start()
        flushes.append(done)

        if k == 0:
            query = queries[l, head]
            scale = 1.0 / math.sqrt(depth)
            for ref, e, lo, hi in parts:
                for f in range(fanout):
                    scores[f * sources + (mine ^ e), :, lo * PAGE : hi * PAGE] = lax.dot_general(
                        query,
                        ref[f].reshape((hi - lo) * PAGE, depth),
                        (((1,), (1,)), ((), ())),
                        preferred_element_type=jnp.float32,
                    )
            fresh_score = jnp.sum(query.astype(jnp.float32) * row, axis=-1, keepdims=True)
            values = jnp.where(places == length, fresh_score[None], scores[...]) * scale
            masked = jnp.where(places <= length, values, -1e30)
            highest = jnp.max(jnp.max(masked, axis=-1, keepdims=True), axis=0, keepdims=True)
            exponent = jnp.where(places <= length, jnp.exp(masked - highest), 0.0)
            total = jnp.sum(jnp.sum(exponent, axis=-1, keepdims=True), axis=0, keepdims=True)
            if l in probs_out:
                probs_out[l][...] = (exponent / total).astype(jnp.bfloat16)
                probs_now[l] = probs_out[l]
        else:
            weights = probs_now[l]
            weighted = sums[group, l][...] if (group, l) in sums else None
            if weighted is None:
                at_fresh = jnp.where(places == length, weights[...].astype(jnp.float32), 0.0)
                share = jnp.sum(jnp.sum(at_fresh, axis=-1, keepdims=True), axis=0)
                weighted = share * row
            for ref, e, lo, hi in parts:
                for f in range(fanout):
                    rank = f * sources + (mine ^ e)
                    mix = weights[rank, :, lo * PAGE : hi * PAGE].astype(jnp.float32)
                    at = lax.broadcasted_iota(jnp.int32, mix.shape, 1)
                    at += rank * blocks * PAGE + lo * PAGE
                    mix = jnp.where(at == length, 0.0, mix).astype(jnp.bfloat16)
                    weighted += jnp.dot(
                        mix,
                        ref[f].reshape((hi - lo) * PAGE, depth),
                        preferred_element_type=jnp.float32,
                    )
            sums[group, l] = weighted
            if l in sums_out:
                sums_out[l][...] = weighted
    if plan["final"]:
        for l in range(queries.shape[0]):
            for h in range(heads):
                mixed = jnp.zeros((per_head, depth), jnp.float32)
                for g in range(heads):
                    picked = (me // sources) ^ g == h
                    mixed = jnp.where(picked, sums[g, l][...], mixed)
                here = pl.ds(h * per_head, per_head)
                attention_out[l, here, :] = mixed.astype(attention_out.dtype)
    for flush in flushes:
        flush.wait()


def head_call(plan, args, operands, probs, sums, pool, pool_shape):
    slots, lengths, queries, fresh, spread = args
    fanout, blocks, _, depth = spread.shape[3:]
    layers, heads, per_head, _ = queries.shape
    units, group, sources = plan["units"], plan["group"], plan["sources"]
    ranks = fanout * sources
    plan = dict(plan, piece=spread.shape[3:], heads=heads, kv_heads=fresh.shape[3])
    plan["operands"] = len(operands)
    plan["has_pool"] = pool is not None
    value_layers = [l for k, l in units if k == 1]
    plan["probs_out"] = [l for k, l in units if k == 0]
    plan["given_probs"] = [l for l in value_layers if l not in plan["probs_out"]]
    if plan["final"]:
        plan["sums_in"], plan["sums_out"] = list(sums), []
    else:
        plan["sums_in"], plan["sums_out"] = [], value_layers
    smem = pl.BlockSpec(memory_space=pltpu.SMEM)
    vmem = pl.BlockSpec(memory_space=pltpu.VMEM)
    anywhere = pl.BlockSpec(memory_space=pl.ANY)
    inputs = [slots, lengths, queries, fresh] + ([spread] if plan["own"] else [])
    in_specs = [smem, smem, vmem, vmem] + (
        [pl.BlockSpec(memory_space=pltpu.HBM)] if plan["own"] else []
    )
    inside = [*operands, *(probs[group, l] for l in plan["given_probs"])]
    inside += [sums[name] for name in plan["sums_in"]]
    inputs += inside
    in_specs += [vmem] * len(inside)
    aliases = {}
    if pool is not None:
        aliases = {len(inputs): 0}
        inputs.append(pool)
        in_specs.append(anywhere)
    prob_shape = jax.ShapeDtypeStruct((ranks, per_head, blocks * PAGE), jnp.bfloat16)
    out_shape = [jax.ShapeDtypeStruct(pool_shape, jnp.bfloat16)]
    out_shape += [prob_shape] * len(plan["probs_out"])
    out_shape += [jax.ShapeDtypeStruct((per_head, depth), jnp.float32)] * len(plan["sums_out"])
    if plan["final"]:
        out_shape.append(jax.ShapeDtypeStruct((layers, heads * per_head, depth), jnp.bfloat16))
    count = len(units)
    own_shape = (count, *spread.shape[3:]) if plan["own"] else (1, 1, 1, PAGE, depth)
    results = list(pl.pallas_call(
        functools.partial(head_kernel, plan),
        out_shape=out_shape,
        in_specs=in_specs,
        out_specs=[anywhere] + [vmem] * (len(out_shape) - 1),
        scratch_shapes=[
            pltpu.VMEM((ranks, per_head, blocks * PAGE), jnp.float32),
            pltpu.VMEM((count, ranks * blocks, PAGE, depth), jnp.bfloat16),
            pltpu.VMEM(own_shape, jnp.bfloat16),
            pltpu.SemaphoreType.DMA((count,)),
            pltpu.SemaphoreType.DMA((count,)),
        ],
        input_output_aliases=aliases,
        compiler_params=pltpu.CompilerParams(vmem_limit_bytes=16 << 20),
        cost_estimate=pl.CostEstimate(
            flops=0, bytes_accessed=count * 4 * ranks * blocks * PAGE * depth * 2, transcendentals=0
        ),
    )(*inputs))
    pool = results.pop(0)
    for l in plan["probs_out"]:
        probs[group, l] = results.pop(0)
    for l in plan["sums_out"]:
        sums[group, l] = results.pop(0)
    return pool, results.pop(0) if plan["final"] else None


def body(tp_ranks, seq_ranks, kv_prefill, queries, new_kv, lengths, page_slots):
    return handoff(tp_ranks, seq_ranks, kv_prefill, queries, new_kv, lengths, page_slots)


def handoff(tp_ranks, seq_ranks, kv_prefill, queries, new_kv, lengths, page_slots):
    kv_heads = new_kv.shape[3]
    layers = kv_prefill.shape[1]
    depth = kv_prefill.shape[4]
    heads = max(1, kv_heads // tp_ranks)
    fanout = tp_ranks * heads // kv_heads
    sources = seq_ranks // heads
    blocks = kv_prefill.shape[3] // PAGE
    pages = page_slots.shape[1]

    spread = spread_heads(kv_prefill, fanout)
    spread = spread.reshape(2, layers, spread.shape[2], fanout, blocks, PAGE, depth)
    units = [(k, l) for k in (0, 1) for l in range(layers)]
    quarter = max(1, blocks // 4)
    far = range(sources, seq_ranks)

    sends = []
    for k, l in units:
        spans = [(0, blocks)]
        if (k, l) == units[0]:
            spans = [(0, quarter), (quarter, blocks)]
        elif (k, l) == units[-1]:
            spans = [(0, blocks - quarter), (blocks - quarter, blocks)]
        for lo, hi in spans:
            stage = 0 if (k, l) == units[0] and lo == 0 else 1
            sends += [(stage, delta, [(k, l, lo, hi)]) for delta in far]
    sends += [(2, delta, [(k, l, 0, blocks) for k, l in units]) for delta in range(1, sources)]
    arrived = []
    after = []
    for stage in range(3):
        batch = [(delta, items) for at, delta, items in sends if at == stage]
        if not batch:
            continue
        wanted = [[(k, l, delta, lo, hi) for k, l, lo, hi in items] for delta, items in batch]
        blocks_out = cut(spread, wanted, after)
        after = [blocks_out[0]]
        for (delta, items), block in zip(batch, blocks_out):
            arrived.append((delta, items, swapped(block, "seq", delta)))

    grouped = queries.reshape(layers, heads, queries.shape[2] // heads, depth)
    args = (page_slots, lengths, grouped, new_kv, spread)
    pool_shape = (2, layers, heads, pages, PAGE, depth)
    probs, sums = {}, {}

    def launch(units, group, chosen, pool, own=False, final=False, close=False):
        parts = [
            (at, row, (k, l), delta - group * sources, lo, hi)
            for at, (delta, items, _) in enumerate(chosen)
            for row, (k, l, lo, hi) in enumerate(items)
        ]
        plan = dict(
            units=units, group=group, sources=sources, parts=parts, own=own, final=final,
            close=close, tp_ranks=tp_ranks,
        )
        operands = [block for _, _, block in chosen]
        return head_call(plan, args, operands, probs, sums, pool, pool_shape)

    near = [a for a in arrived if a[0] < sources]
    pool, out = launch(units, 0, near, None, own=True, final=heads == 1)
    for group in range(1, heads):
        for unit in units:
            chosen = [a for a in arrived if a[0] // sources == group and a[1][0][:2] == unit]
            if unit == units[-1]:
                early = [a for a in chosen if a[1][0][2] == 0]
                pool, _ = launch([unit], group, early, pool)
                chosen = [a for a in chosen if a[1][0][2] > 0]
                pool, out = launch(
                    [unit], group, chosen, pool, final=group == heads - 1, close=True
                )
            else:
                pool, _ = launch([unit], group, chosen, pool)
    return pool, out.reshape(queries.shape)


def solution(mesh):
    placed = (
        P(None, None, "groups", ("tp", "seq"), None),
        P(None, ("groups", "seq"), "tp", None),
        P(None, None, ("groups", "seq"), None, None),
        P(("groups", "seq")),
        P(("groups", "seq"), None),
    )
    return jax.shard_map(
        functools.partial(body, mesh.shape["tp"], mesh.shape["seq"]),
        mesh=mesh,
        in_specs=placed,
        out_specs=(
            P(None, None, "tp", ("groups", "seq"), None, None),
            P(None, ("groups", "seq"), "tp", None),
        ),
        check_vma=False,
    )
```

```python
import functools
import math

import jax
import jax.numpy as jnp
from jax import lax
from jax.experimental import pallas as pl
from jax.experimental.pallas import tpu as pltpu
from jax.sharding import PartitionSpec as P


PAGE = 16
UNROLL = 16
VMEM = 67_043_328


def swapped(array, axis, bits):
    return lax.ppermute(array, axis, [(i, i ^ bits) for i in range(lax.axis_size(axis))])


def spread_heads(blocks, fanout):
    rank = lax.axis_index("tp")
    for bit in range(fanout.bit_length() - 1):
        partner = swapped(blocks, "tp", 1 << bit)
        lower = rank // (1 << bit) % 2 == 0
        pair = (jnp.where(lower, blocks, partner), jnp.where(lower, partner, blocks))
        blocks = jnp.concatenate(pair, axis=3)
    return blocks


def cut_kernel(wanted, *refs):
    spread, outs, sems = refs[0], refs[-1 - len(wanted) : -1], refs[-1]
    me = lax.axis_index("seq")
    copies = []
    for out, items in zip(outs, wanted):
        for n, (k, l, delta, lo, hi) in enumerate(items):
            source = spread.at[k, l, me ^ delta, :, lo:hi]
            copies.append(pltpu.make_async_copy(source, out.at[n], sems.at[len(copies)]))
            copies[-1].start()
    for copy in copies:
        copy.wait()


def cut(spread, wanted, after, room):
    fanout, _, page, depth = spread.shape[3:]
    shapes = [
        jax.ShapeDtypeStruct((len(w), fanout, w[0][4] - w[0][3], page, depth), spread.dtype)
        for w in wanted
    ]
    anywhere = pl.BlockSpec(memory_space=pl.ANY)
    return pl.pallas_call(
        functools.partial(cut_kernel, wanted),
        out_shape=shapes,
        in_specs=[pl.BlockSpec(memory_space=pltpu.HBM)] + [anywhere] * len(after),
        out_specs=[pl.BlockSpec(memory_space=pltpu.VMEM)] * len(shapes),
        scratch_shapes=[pltpu.SemaphoreType.DMA((sum(len(w) for w in wanted),))],
        compiler_params=pltpu.CompilerParams(vmem_limit_bytes=VMEM - room),
        cost_estimate=pl.CostEstimate(
            flops=0, bytes_accessed=2 * sum(2 * math.prod(o.shape) for o in shapes), transcendentals=0
        ),
    )(spread, *after)


def head_kernel(plan, *refs):
    refs = list(refs)

    def take(count):
        return [refs.pop(0) for _ in range(count)]

    units, group, sources = plan["units"], plan["group"], plan["sources"]
    slots, lengths, queries, fresh = take(4)
    operands = take(plan["operands"])
    given_probs = dict(zip(plan["given_probs"], take(len(plan["given_probs"]))))
    sums_in = dict(zip(plan["sums_in"], take(len(plan["sums_in"]))))
    if plan["has_pool"]:
        take(1)
    (pool,) = take(1)
    probs_out = dict(zip(plan["probs_out"], take(len(plan["probs_out"]))))
    sums_out = dict(zip(plan["sums_out"], take(len(plan["sums_out"]))))
    attention_out = take(1)[0] if plan["final"] else None
    scores, paged, mixed_buf, mixed_sem, out_sems = refs

    me = lax.axis_index("seq")
    mine = me % sources
    head = (me // sources) ^ group
    heads = plan["heads"]
    first = lax.axis_index("tp") * plan["kv_heads"] // plan["tp_ranks"]
    fanout, blocks, _, depth = plan["piece"]
    length = lengths[0]
    per_head = queries.shape[2]
    places = lax.broadcasted_iota(jnp.int32, scores.shape, 0) * (blocks * PAGE)
    places += lax.broadcasted_iota(jnp.int32, scores.shape, 2)
    probs_now = dict(given_probs)
    sums = dict(sums_in)
    flushes = []
    for n, (k, l) in enumerate(units):
        parts = [
            (operands[at].at[row], e, lo, hi)
            for at, row, unit, e, lo, hi in plan["parts"]
            if unit == (k, l)
        ]
        rows = fresh[k, l, 0].astype(jnp.float32)
        row_at = lax.broadcasted_iota(jnp.int32, rows.shape, 0)
        row = jnp.sum(jnp.where(row_at == first + head, rows, 0.0), axis=0, keepdims=True)

        def patched(page):
            offset = lax.broadcasted_iota(jnp.int32, page.shape, 0)
            return jnp.where(offset == length % PAGE, row, page.astype(jnp.float32)).astype(page.dtype)

        if plan["close"]:
            count = 0
            for ref, e, lo, hi in parts:
                for f in range(fanout):
                    base = (f * sources + (mine ^ e)) * blocks + lo
                    paged[n, count : count + hi - lo] = ref[f]
                    inside = (length // PAGE >= base) & (length // PAGE < base + hi - lo)

                    @pl.when(inside)
                    def _():
                        at = count + length // PAGE - base
                        paged[n, at] = patched(paged[n, at])

                    for b in range(hi - lo):
                        pltpu.make_async_copy(
                            paged.at[n, count + b],
                            pool.at[k, l, head, slots[0, base + b]],
                            out_sems.at[n],
                        ).start()
                    count += hi - lo
            done = pltpu.make_async_copy(
                paged.at[n, :count], pool.at[k, l, head, :count], out_sems.at[n]
            )
        else:
            for ref, e, lo, hi in parts:
                for f in range(fanout):
                    base = (f * sources + (mine ^ e)) * blocks + lo
                    unroll = math.gcd(UNROLL, hi - lo)

                    def move(step, carry, ref=ref, f=f, base=base, unroll=unroll):
                        start = step * unroll
                        held = [ref[f, start + i] for i in range(unroll)]
                        for i in range(unroll):
                            paged[n, slots[0, base + start + i]] = held[i]
                        return carry

                    lax.fori_loop(0, (hi - lo) // unroll, move, 0)
            spot = slots[0, length // PAGE]
            paged[n, spot] = patched(paged[n, spot])
            done = pltpu.make_async_copy(paged.at[n], pool.at[k, l, head], out_sems.at[n])
            done.start()
        flushes.append(done)

        if k == 0:
            query = queries[l, head]
            scale = 1.0 / math.sqrt(depth)
            for ref, e, lo, hi in parts:
                for f in range(fanout):
                    scores[f * sources + (mine ^ e), :, lo * PAGE : hi * PAGE] = lax.dot_general(
                        query,
                        ref[f].reshape((hi - lo) * PAGE, depth),
                        (((1,), (1,)), ((), ())),
                        preferred_element_type=jnp.float32,
                    )
            fresh_score = jnp.sum(query.astype(jnp.float32) * row, axis=-1, keepdims=True)
            values = jnp.where(places == length, fresh_score[None], scores[...]) * scale
            masked = jnp.where(places <= length, values, -1e30)
            highest = jnp.max(jnp.max(masked, axis=-1, keepdims=True), axis=0, keepdims=True)
            exponent = jnp.where(places <= length, jnp.exp(masked - highest), 0.0)
            total = jnp.sum(jnp.sum(exponent, axis=-1, keepdims=True), axis=0, keepdims=True)
            if l in probs_out:
                probs_out[l][...] = (exponent / total).astype(jnp.bfloat16)
                probs_now[l] = probs_out[l]
        else:
            weights = probs_now[l]
            weighted = sums[group, l][...] if (group, l) in sums else None
            if weighted is None:
                at_fresh = jnp.where(places == length, weights[...].astype(jnp.float32), 0.0)
                share = jnp.sum(jnp.sum(at_fresh, axis=-1, keepdims=True), axis=0)
                weighted = share * row
            for ref, e, lo, hi in parts:
                for f in range(fanout):
                    rank = f * sources + (mine ^ e)
                    mix = weights[rank, :, lo * PAGE : hi * PAGE].astype(jnp.float32)
                    at = lax.broadcasted_iota(jnp.int32, mix.shape, 1)
                    at += rank * blocks * PAGE + lo * PAGE
                    mix = jnp.where(at == length, 0.0, mix).astype(jnp.bfloat16)
                    weighted += jnp.dot(
                        mix,
                        ref[f].reshape((hi - lo) * PAGE, depth),
                        preferred_element_type=jnp.float32,
                    )
            sums[group, l] = weighted
            if l in sums_out:
                sums_out[l][...] = weighted
    if plan["final"]:
        for l in range(queries.shape[0]):
            for h in range(heads):
                mixed = jnp.zeros((per_head, depth), jnp.float32)
                for g in range(heads):
                    picked = (me // sources) ^ g == h
                    mixed = jnp.where(picked, sums[g, l][...], mixed)
                here = pl.ds(h * per_head, per_head)
                mixed_buf[l, here, :] = mixed.astype(mixed_buf.dtype)
        flushes.append(pltpu.make_async_copy(mixed_buf, attention_out, mixed_sem))
        flushes[-1].start()
    for flush in flushes:
        flush.wait()


def head_call(plan, args, operands, probs, sums, pool, pool_shape):
    slots, lengths, queries, fresh = args
    fanout, blocks, _, depth = plan["piece"]
    layers, heads, per_head, _ = queries.shape
    units, group, sources = plan["units"], plan["group"], plan["sources"]
    ranks = fanout * sources
    plan = dict(plan, heads=heads, kv_heads=fresh.shape[3])
    plan["operands"] = len(operands)
    plan["has_pool"] = pool is not None
    value_layers = [l for k, l in units if k == 1]
    plan["probs_out"] = [l for k, l in units if k == 0]
    plan["given_probs"] = [l for l in value_layers if l not in plan["probs_out"]]
    if plan["final"]:
        plan["sums_in"], plan["sums_out"] = list(sums), []
    else:
        plan["sums_in"], plan["sums_out"] = [], value_layers
    smem = pl.BlockSpec(memory_space=pltpu.SMEM)
    vmem = pl.BlockSpec(memory_space=pltpu.VMEM)
    anywhere = pl.BlockSpec(memory_space=pl.ANY)
    inputs = [slots, lengths, queries, fresh]
    in_specs = [smem, smem, vmem, vmem]
    inside = [*operands, *(probs[group, l] for l in plan["given_probs"])]
    inside += [sums[name] for name in plan["sums_in"]]
    inputs += inside
    in_specs += [vmem] * len(inside)
    aliases = {}
    if pool is not None:
        aliases = {len(inputs): 0}
        inputs.append(pool)
        in_specs.append(anywhere)
    prob_shape = jax.ShapeDtypeStruct((ranks, per_head, blocks * PAGE), jnp.bfloat16)
    out_shape = [jax.ShapeDtypeStruct(pool_shape, jnp.bfloat16)]
    out_shape += [prob_shape] * len(plan["probs_out"])
    out_shape += [jax.ShapeDtypeStruct((per_head, depth), jnp.float32)] * len(plan["sums_out"])
    if plan["final"]:
        out_shape.append(jax.ShapeDtypeStruct((layers, heads * per_head, depth), jnp.bfloat16))
    count = len(units)
    out_specs = [anywhere] + [vmem] * (len(out_shape) - 1)
    if plan["final"]:
        out_specs[-1] = anywhere
    results = list(pl.pallas_call(
        functools.partial(head_kernel, plan),
        out_shape=out_shape,
        in_specs=in_specs,
        out_specs=out_specs,
        scratch_shapes=[
            pltpu.VMEM((ranks, per_head, blocks * PAGE), jnp.float32),
            pltpu.VMEM((count, ranks * blocks, PAGE, depth), jnp.bfloat16),
            pltpu.VMEM((layers, heads * per_head, depth), jnp.bfloat16),
            pltpu.SemaphoreType.DMA,
            pltpu.SemaphoreType.DMA((count,)),
        ],
        input_output_aliases=aliases,
        compiler_params=pltpu.CompilerParams(vmem_limit_bytes=16 << 20),
        cost_estimate=pl.CostEstimate(
            flops=0, bytes_accessed=count * 4 * ranks * blocks * PAGE * depth * 2, transcendentals=0
        ),
    )(*inputs))
    pool = results.pop(0)
    for l in plan["probs_out"]:
        probs[group, l] = results.pop(0)
    for l in plan["sums_out"]:
        sums[group, l] = results.pop(0)
    return pool, results.pop(0) if plan["final"] else None


def body(tp_ranks, seq_ranks, kv_prefill, queries, new_kv, lengths, page_slots):
    return handoff(tp_ranks, seq_ranks, kv_prefill, queries, new_kv, lengths, page_slots)


def handoff(tp_ranks, seq_ranks, kv_prefill, queries, new_kv, lengths, page_slots):
    kv_heads = new_kv.shape[3]
    layers = kv_prefill.shape[1]
    depth = kv_prefill.shape[4]
    heads = max(1, kv_heads // tp_ranks)
    fanout = tp_ranks * heads // kv_heads
    sources = seq_ranks // heads
    blocks = kv_prefill.shape[3] // PAGE
    pages = page_slots.shape[1]

    spread = spread_heads(kv_prefill, fanout)
    spread = spread.reshape(2, layers, spread.shape[2], fanout, blocks, PAGE, depth)
    units = [(k, l) for k in (0, 1) for l in range(layers)]
    head_span = max(1, blocks // 4)
    tail_span = max(1, blocks // 8)
    far = range(sources, seq_ranks)

    sends = []
    for k, l in units:
        spans = [(0, blocks)]
        if (k, l) == units[0]:
            spans = [(0, head_span), (head_span, blocks)]
        elif (k, l) == units[-1]:
            spans = [(0, blocks - tail_span), (blocks - tail_span, blocks)]
        for lo, hi in spans:
            stage = 0 if (k, l) == units[0] and lo == 0 else 1
            sends += [(stage, delta, [(k, l, lo, hi)]) for delta in far]
    sends += [(2, delta, [(k, l, 0, blocks) for k, l in units]) for delta in range(sources)]
    arrived = []
    after = []
    for stage in range(3):
        batch = [(delta, items) for at, delta, items in sends if at == stage]
        if not batch:
            continue
        wanted = [[(k, l, delta, lo, hi) for k, l, lo, hi in items] for delta, items in batch]
        room = (11 << 20, 15 << 20, 24 << 20)[stage]
        blocks_out = cut(spread, wanted, after, room)
        after = [blocks_out[0]]
        for (delta, items), block in zip(batch, blocks_out):
            moved = swapped(block, "seq", delta) if delta > 0 else block
            arrived.append((delta, items, moved))

    grouped = queries.reshape(layers, heads, queries.shape[2] // heads, depth)
    args = (page_slots, lengths, grouped, new_kv)
    pool_shape = (2, layers, heads, pages, PAGE, depth)
    probs, sums = {}, {}

    def launch(units, group, chosen, pool, final=False, close=False):
        parts = [
            (at, row, (k, l), delta - group * sources, lo, hi)
            for at, (delta, items, _) in enumerate(chosen)
            for row, (k, l, lo, hi) in enumerate(items)
        ]
        plan = dict(
            units=units, group=group, sources=sources, parts=parts, final=final,
            close=close, tp_ranks=tp_ranks, piece=spread.shape[3:],
        )
        operands = [block for _, _, block in chosen]
        return head_call(plan, args, operands, probs, sums, pool, pool_shape)

    near = [a for a in arrived if a[0] < sources]
    pool, out = launch(units, 0, near, None, final=heads == 1)
    for group in range(1, heads):
        for unit in units:
            chosen = [a for a in arrived if a[0] // sources == group and a[1][0][:2] == unit]
            if unit == units[-1]:
                early = [a for a in chosen if a[1][0][2] == 0]
                pool, _ = launch([unit], group, early, pool)
                chosen = [a for a in chosen if a[1][0][2] > 0]
                pool, out = launch(
                    [unit], group, chosen, pool, final=group == heads - 1, close=True
                )
            else:
                pool, _ = launch([unit], group, chosen, pool)
    return pool, out.reshape(queries.shape)


def solution(mesh):
    placed = (
        P(None, None, "groups", ("tp", "seq"), None),
        P(None, ("groups", "seq"), "tp", None),
        P(None, None, ("groups", "seq"), None, None),
        P(("groups", "seq")),
        P(("groups", "seq"), None),
    )
    return jax.shard_map(
        functools.partial(body, mesh.shape["tp"], mesh.shape["seq"]),
        mesh=mesh,
        in_specs=placed,
        out_specs=(
            P(None, None, "tp", ("groups", "seq"), None, None),
            P(None, ("groups", "seq"), "tp", None),
        ),
        check_vma=False,
    )
```
